32 devices in a mesh: gx: 8 (over y, x, core), gy: 4 (over z).
Axes of the slice: x: 2, y: 2, z: 4, core: 2. Of those that a mesh axis runs over, the one named last changes fastest.
Arguments:
- volts: float32 [32, 4, 64, 512], P(None, None, 'gx', 'gy'), may hold values from -6 to 6
- cap: float32 [4, 64, 512], P(None, 'gx', 'gy'), may hold values from 0.05 to 1
- cond_x: float32 [4, 64, 512], P(None, 'gx', 'gy'), may hold values from 0.5 to 2
- cond_y: float32 [4, 64, 512], P(None, 'gx', 'gy'), may hold values from 0.5 to 2
- via: float32 [4, 64, 512], P(None, 'gx', 'gy'), may hold values from 0.2 to 2
- waveforms: float32 [64, 64], replicated, may hold values from -6 to 6
- placement: int32 [262144, 1], P(('gx', 'gy')), may hold values from 0 to 31; in each aligned block of 8192 rows (0 to 8191, 8192 to 16383, ...) at most 512 rows name the same one
- cells: int32 [262144], P(('gx', 'gy')), may hold values from 0 to 1023
- wave_ids: int32 [262144], P(('gx', 'gy')), may hold values from 0 to 63
- amps: float32 [262144], P(('gx', 'gy')), may hold values from 0.5 to 4
Outputs:
- volts_out: float32 [32, 4, 64, 512], P(None, None, 'gx', 'gy')
- residual: float32 [32, 4, 64, 512], P(None, None, 'gx', 'gy')
The draws below stay inside these ranges and needn't reach their ends.
Inputs may be any that keep to these rules, and one draw needn't show every extreme that they name: `placement`: in each device's block of 8192 rows no tile is named more than 512 times, a bound that some block reaches.
All inputs are finite; a program needn't handle non-finite values.
Results may differ from the reference program's by a relative error of at most 0.0029.
Values may be sent and summed in bfloat16 or wider, within the bound.
A program may use at most 64 MiB of HBM per device.

```python
import math
import jax
import jax.numpy as jnp
import numpy as np
from jax import lax

SCEN = 32
LAYERS = 4
WAVES = 64
CX = 8
CY = 128
INST_DEV = 8192
STEPS = 2
ITERS = 3
CAP = 512
INSTANCES = 262144
NX = 64
NY = 512
N_GY = 4
DEVICES = 32


def touch_ends(drawn, key, least, largest):
    place = [jax.random.randint(jax.random.fold_in(key, axis), (), 0, length) for axis, length in enumerate(drawn.shape)]
    widest = drawn.shape.index(max(drawn.shape))
    beside = place[:widest] + [(place[widest] + 1) % drawn.shape[widest]] + place[widest + 1:]
    return drawn.at[tuple(place)].set(least).at[tuple(beside)].set(largest)


def steps_of(rng, dims, shards, smallest, high):
    def one(axis_at, parts):
        draws = jax.random.uniform(jax.random.fold_in(jax.random.fold_in(rng, 6), axis_at), (parts,), jnp.float32, smallest / len(shards), high / len(shards))
        return jnp.repeat(jnp.exp(draws), dims[axis_at] // parts).reshape((-1,) + (1,) * (len(dims) - axis_at - 1))

    factor_of = one(*shards[0])
    for cut in shards[1:]:
        factor_of = factor_of * one(*cut)
    return factor_of


def assign_block(rng, own, number, rows, number_of, top, limit, slope):
    order = jax.random.permutation(rng, number_of)
    heavy_load, usual = shares(number_of, rows * top, limit, slope, True), shares(number_of, rows * top, limit, slope, False)
    places = jnp.arange(number_of)

    def named(tallies, rotation):
        used = int((tallies > 0).sum())
        fixed = max(1, used // 4)
        passed = fixed + (places - fixed + rotation * (used - fixed)) % max(1, number_of - fixed)
        return jnp.zeros((number_of,), jnp.int32).at[order[jnp.where(places < fixed, places, passed)]].set(jnp.asarray(tallies, jnp.int32))

    tallies = jnp.where(number % 4 == 0, named(heavy_load, number // 4), named(usual, number - number // 4 - 1))
    mixed = jax.random.permutation(jax.random.fold_in(own, 3), number_of)
    donor, taker = mixed[0:number_of // 2 * 2:2], mixed[1:number_of // 2 * 2:2]
    slack = jnp.minimum(tallies[donor] - 1, limit - tallies[taker]) // 2
    slack = jnp.where((donor == order[0]) | (taker == order[0]) | (tallies[taker] == 0), 0, jnp.maximum(slack, 0))
    passed = jax.random.randint(jax.random.fold_in(own, 4), (number_of // 2,), 0, 1 << 20) % (slack + 1)
    tallies = tallies.at[donor].add(-passed).at[taker].add(passed)
    labels = jnp.searchsorted(jnp.cumsum(tallies), jnp.arange(rows * top), side="right").astype(jnp.int32)
    grid = labels.reshape(top, rows).T
    grid = grid[jax.random.permutation(jax.random.fold_in(own, 1), rows)]
    rotation = jax.random.randint(jax.random.fold_in(own, 2), (rows, 1), 0, top)
    return jnp.take_along_axis(grid, (jnp.arange(top)[None, :] + rotation) % top, axis=1)


def shares(number_of, total, limit, slope, full):
    loads = [(1 << 20) // math.isqrt(grade ** slope) + 1 for grade in range(1, number_of + 1)]
    largest = limit if full else min(limit, max(-(-total // number_of), total * loads[0] // sum(loads)))
    least = 1 if total - largest >= number_of - 1 else 0
    counts, rest = [largest] + [least] * (number_of - 1), total - largest - least * (number_of - 1)
    while rest > 0:
        free = [i for i in range(1, number_of) if counts[i] < largest] or [i for i in range(1, number_of) if counts[i] < limit]
        mass, left = sum([loads[i] for i in free]), rest
        for i in free:
            more = min(limit - counts[i], max(1, left * loads[i] // mass), rest)
            counts[i] = counts[i] + more
            rest = rest - more
    return np.array(counts)


def normal_values(stream_key, shape, spread, most, split=(), held_as=jnp.bfloat16):
    values = spread * jax.random.normal(stream_key, shape, jnp.float32)
    if split:
        values = values * steps_of(stream_key, shape, split, -0.22, 0.18)
    return jnp.clip(values, -most, most).astype(held_as)


def setup_inputs(seed: int = 0) -> dict:
    arg_keys = jax.random.split(jax.random.key(seed), 11)
    volts = normal_values(arg_keys[0], (SCEN, LAYERS, NX, NY), 1.0, 6.0, ((2, 8), (3, 4)), jnp.float32)
    cap = jnp.clip(jnp.exp(math.log(1.0) - 2.9957323 * jax.random.uniform(arg_keys[1], (LAYERS, NX, NY), jnp.float32) ** steps_of(arg_keys[1], (LAYERS, NX, NY), ((1, 8), (2, 4)), -0.2, 0.2)), 0.05, 1.0)
    cond_x = jnp.clip(jnp.exp(math.log(2.0) - 1.3862944 * jax.random.uniform(arg_keys[2], (LAYERS, NX, NY), jnp.float32) ** steps_of(arg_keys[2], (LAYERS, NX, NY), ((1, 8), (2, 4)), -0.2, 0.2)), 0.5, 2.0)
    cond_y = jnp.clip(jnp.exp(math.log(2.0) - 1.3862944 * jax.random.uniform(arg_keys[3], (LAYERS, NX, NY), jnp.float32) ** steps_of(arg_keys[3], (LAYERS, NX, NY), ((1, 8), (2, 4)), -0.2, 0.2)), 0.5, 2.0)
    via = jnp.clip(jnp.exp(math.log(2.0) - 2.3025851 * jax.random.uniform(arg_keys[4], (LAYERS, NX, NY), jnp.float32) ** steps_of(arg_keys[4], (LAYERS, NX, NY), ((1, 8), (2, 4)), -0.2, 0.2)), 0.2, 2.0)
    waveforms = normal_values(arg_keys[5], (STEPS * SCEN, WAVES), 1.0, 6.0, (), jnp.float32)
    placement_keys = jax.random.split(jax.random.fold_in(arg_keys[6], 1), INSTANCES // INST_DEV)
    placement_turns = jax.random.permutation(jax.random.fold_in(arg_keys[6], 3), INSTANCES // INST_DEV)
    placement = jax.vmap(lambda own, number: assign_block(jax.random.fold_in(arg_keys[6], 2), own, number, INST_DEV, DEVICES, 1, CAP, 2))(placement_keys, placement_turns).reshape((INSTANCES, 1))
    cells = touch_ends(jax.random.randint(arg_keys[7], (INSTANCES,), 0, CX * CY), jax.random.fold_in(arg_keys[7], 1), 0, (CX * CY) - 1).astype(jnp.int32)
    wave_ids = touch_ends(jax.random.randint(arg_keys[8], (INSTANCES,), 0, WAVES), jax.random.fold_in(arg_keys[8], 1), 0, WAVES - 1).astype(jnp.int32)
    amps = jnp.clip(jnp.exp(math.log(4.0) - 2.0794415 * jax.random.uniform(arg_keys[9], (INSTANCES,), jnp.float32) ** steps_of(arg_keys[9], (INSTANCES,), ((0, 32),), -0.2, 0.2)), 0.5, 4.0)
    return dict(volts=volts, cap=cap, cond_x=cond_x, cond_y=cond_y, via=via, waveforms=waveforms, placement=placement, cells=cells, wave_ids=wave_ids, amps=amps)


def operate(field, cap, cond_x, cond_y, via):
    cond_x_low = jnp.pad(cond_x, ((0, 0), (1, 0), (0, 0)))[:, :-1, :]
    cond_y_low = jnp.pad(cond_y, ((0, 0), (0, 0), (1, 0)))[:, :, :-1]
    via_low = jnp.pad(via, ((1, 0), (0, 0), (0, 0)))[:-1]
    padded = jnp.pad(field, ((0, 0), (0, 0), (1, 1), (1, 1)))
    upper = jnp.pad(field, ((0, 0), (0, 1), (0, 0), (0, 0)))[:, 1:]
    lower = jnp.pad(field, ((0, 0), (1, 0), (0, 0), (0, 0)))[:, :-1]
    result = cap * field
    result = result + cond_x * (field - padded[:, :, 2:, 1:-1])
    result = result + cond_x_low * (field - padded[:, :, :-2, 1:-1])
    result = result + cond_y * (field - padded[:, :, 1:-1, 2:])
    result = result + cond_y_low * (field - padded[:, :, 1:-1, :-2])
    result = result + via * (field - upper) + via_low * (field - lower)
    return result

def gram(left, right):
    left_rows = left.reshape(left.shape[0], -1)
    right_rows = right.reshape(right.shape[0], -1)
    return lax.dot_general(left_rows, right_rows, (((1,), (1,)), ((), ())), precision=lax.Precision.HIGHEST)

def combine(coef, field):
    return jnp.einsum('st,slxy->tlxy', coef, field, precision=lax.Precision.HIGHEST)

def spd_solve(matrix, right):
    factor = jnp.linalg.cholesky(matrix)
    return jax.scipy.linalg.cho_solve((factor, True), right)

def reference(volts, cap, cond_x, cond_y, via, waveforms, placement, cells, wave_ids, amps):
    tile = placement[:, 0]
    row_x = tile // N_GY * CX + cells // CY
    col_y = tile % N_GY * CY + cells % CY
    flat = (row_x * NY + col_y).astype(jnp.int32)
    currents = (waveforms[:, wave_ids] * amps[None, :]).astype(jnp.bfloat16)
    injected = jax.ops.segment_sum(currents.astype(jnp.float32).T, flat, num_segments=NX * NY)
    injected = injected.T.reshape(STEPS, SCEN, NX, NY)
    voltage = volts
    residual = volts
    for step in range(STEPS):
        rhs = cap * voltage
        rhs = rhs.at[:, 0].add(-injected[step])
        iterate = voltage
        residual = rhs - operate(iterate, cap, cond_x, cond_y, via)
        direction = residual
        norm_gram = gram(residual, residual)
        for sweep in range(ITERS):
            image = operate(direction, cap, cond_x, cond_y, via)
            curve_gram = gram(direction, image)
            step_coef = spd_solve(curve_gram, norm_gram)
            iterate = iterate + combine(step_coef, direction)
            residual = residual - combine(step_coef, image)
            if sweep + 1 < ITERS:
                new_gram = gram(residual, residual)
                turn_coef = spd_solve(norm_gram, new_gram)
                direction = residual + combine(turn_coef, direction)
                norm_gram = new_gram
        voltage = iterate
    return (voltage, residual)
```

```python
import functools

import jax
import jax.numpy as jnp
from jax import lax
from jax.experimental import pallas as pl
from jax.experimental.pallas import tpu as pltpu
from jax.sharding import PartitionSpec as P

ITERS = 3
LANES = 128
MESH = pl.DeviceIdType.MESH
HIGHEST = lax.Precision.HIGHEST
NT = (((1,), (1,)), ((), ()))
TN = (((0,), (0,)), ((), ()))
F32 = jnp.float32
BF16 = jnp.bfloat16


def split3(x):
    first = x.astype(BF16).astype(F32)
    rest = x - first
    second = rest.astype(BF16).astype(F32)
    return first, second, rest - second


def rows_iota(rows, cols):
    return lax.broadcasted_iota(jnp.int32, (rows, cols), 0)


def bin_kernel(devices, capacity, target_ref, cell_ref, wave_ref, amp_ref, out_ref, acc_ref):
    blocks, width = target_ref.shape
    rows = out_ref.shape[1]
    before = (
        rows_iota(width, width) < lax.broadcasted_iota(jnp.int32, (width, width), 1)
    ).astype(F32).astype(BF16)
    acc_ref[...] = jnp.zeros_like(acc_ref)

    def step(b, base):
        target = target_ref[pl.ds(b, 1), :]
        hits = (rows_iota(devices, width) == target).astype(F32)
        ahead = jnp.dot(hits.astype(BF16), before, preferred_element_type=F32)
        position = jnp.sum(hits * (ahead + base), axis=0, keepdims=True)
        slot = target * capacity + position.astype(jnp.int32)
        row_hits = rows_iota(rows, width) == (slot >> 7)
        lane_hits = (rows_iota(LANES, width) == (slot & 127)).astype(F32).astype(BF16)
        code = cell_ref[pl.ds(b, 1), :] * 64 + wave_ref[pl.ds(b, 1), :]
        parts = split3(amp_ref[pl.ds(b, 1), :]) + (
            (code >> 8).astype(F32),
            (code & 255).astype(F32),
        )
        for i, part in enumerate(parts):
            left = jnp.where(row_hits, part, 0.0).astype(BF16)
            acc_ref[i] += lax.dot_general(left, lane_hits, NT, preferred_element_type=F32)
        return base + jnp.sum(hits, axis=1, keepdims=True)

    lax.fori_loop(0, blocks, step, jnp.zeros((devices, 1), F32), unroll=2)
    out_ref[0] = (acc_ref[2] + acc_ref[1]) + acc_ref[0]
    out_ref[1] = acc_ref[3] * 256.0 + acc_ref[4]


def bin_instances(devices, capacity, target, cells, wave_ids, amps):
    width = 512
    shape = (target.shape[0] // width, width)
    rows = devices * capacity // LANES
    return pl.pallas_call(
        functools.partial(bin_kernel, devices, capacity),
        out_shape=jax.ShapeDtypeStruct((2, rows, LANES), F32),
        in_specs=[pl.BlockSpec(memory_space=pltpu.VMEM)] * 4,
        out_specs=pl.BlockSpec(memory_space=pltpu.VMEM),
        scratch_shapes=[pltpu.VMEM((5, rows, LANES), F32)],
        name="bin",
    )(*[x.reshape(shape) for x in (target, cells, wave_ids, amps)])


def inject_kernel(parts, arrived_ref, wave_ref, out_ref, acc_ref):
    sources, width = arrived_ref.shape[1:]
    kinds = wave_ref.shape[1]
    outs = wave_ref.shape[0]
    low_count = out_ref.shape[1] // parts
    table = jnp.concatenate(split3(wave_ref[...]), axis=0).astype(BF16)
    acc_ref[...] = jnp.zeros_like(acc_ref)

    def step(i, carry):
        amp = arrived_ref[0, pl.ds(i, 1), :]
        code = arrived_ref[1, pl.ds(i, 1), :].astype(jnp.int32)
        cell = code >> 6
        low, high = cell % low_count, cell // low_count
        kind_hits = (rows_iota(kinds, width) == (code & 63)).astype(F32).astype(BF16)
        picked = jnp.dot(table, kind_hits, preferred_element_type=F32)
        wave = (picked[2 * outs :] + picked[outs : 2 * outs]) + picked[:outs]
        currents = (wave * amp).astype(BF16).astype(F32)
        low_hits = (rows_iota(low_count, width) == low).astype(F32).astype(BF16)
        left = jnp.concatenate(
            [jnp.where(high == h, currents, 0.0).astype(BF16) for h in range(parts)], axis=0
        )
        acc_ref[...] += lax.dot_general(left, low_hits, NT, preferred_element_type=F32)
        return carry

    lax.fori_loop(0, sources, step, 0, unroll=2)
    for h in range(parts):
        out_ref[:, h * low_count : (h + 1) * low_count] = acc_ref[h * outs : (h + 1) * outs]


def inject(arrived, waveforms, die_cells):
    parts = 4
    return pl.pallas_call(
        functools.partial(inject_kernel, parts),
        out_shape=jax.ShapeDtypeStruct((waveforms.shape[0], die_cells), F32),
        in_specs=[pl.BlockSpec(memory_space=pltpu.VMEM)] * 2,
        out_specs=pl.BlockSpec(memory_space=pltpu.VMEM),
        scratch_shapes=[pltpu.VMEM((parts * waveforms.shape[0], die_cells // parts), F32)],
        name="inject",
    )(arrived, waveforms)


def eliminate(mats):
    size = mats[0].shape[0]
    rows = rows_iota(size, mats[0].shape[1])
    for k in range(size):
        fresh = []
        for m in mats:
            row = m[k : k + 1, :] / m[k : k + 1, k : k + 1]
            fresh.append(jnp.where(rows == k, row, m - m[:, k : k + 1] * row))
        mats = fresh
    return mats


def beside(left, right):
    size = left.shape[0]
    return jnp.concatenate([left, right, jnp.zeros((size, LANES - 2 * size), F32)], axis=1)


def small(a, b, dims=(((1,), (0,)), ((), ()))):
    return lax.dot_general(a, b, dims, precision=HIGHEST, preferred_element_type=F32)


def grid_kernel(
    nx, ny, steps, layers, tile_x,
    v_in, inj, coef, v, r,
    d, image, xs, xl, ys, yl, gs, gl, hs, hl,
    xsend, xrecv, ysend, yrecv, gsend, grecv, hsend, hrecv,
):
    gx, gy = lax.axis_index("gx"), lax.axis_index("gy")
    size = v.shape[0]
    count = layers * tile_x
    lane = lax.broadcasted_iota(jnp.int32, (size, LANES), 1)

    barrier = pltpu.get_barrier_semaphore()
    for axis, me, n in (("gx", gx, nx), ("gy", gy, ny)):
        for j in range(1, n):
            pl.semaphore_signal(
                barrier, inc=1, device_id={axis: lax.rem(me + j, n)}, device_id_type=MESH
            )
    pl.semaphore_wait(barrier, nx + ny - 2)

    def block(ref, c):
        return ref[:, c * LANES : (c + 1) * LANES]

    def exchange(src, e):
        for l in range(layers):
            at = slice(l * LANES, (l + 1) * LANES)
            xs[e, 0, :, at] = block(src, l * tile_x + tile_x - 1)
            xs[e, 1, :, at] = block(src, l * tile_x)
        copies = []
        for side, step in ((0, 1), (1, nx - 1)):
            copies.append(pltpu.make_async_remote_copy(
                xs.at[e, side], xl.at[e, side], xsend.at[e, side], xrecv.at[e, side],
                device_id={"gx": lax.rem(gx + step, nx)}, device_id_type=MESH,
            ))
            copies[-1].start()
        last = jnp.zeros((size, LANES), F32)
        first = last
        for c in range(count):
            f = block(src, c)
            last = jnp.where(lane == c, pltpu.roll(f, (c + 1) % LANES, 1), last)
            first = jnp.where(lane == c, pltpu.roll(f, c, 1) if c else f, first)
        ys[e, 0] = last
        ys[e, 1] = first
        for side, step in ((0, 1), (1, ny - 1)):
            copies.append(pltpu.make_async_remote_copy(
                ys.at[e, side], yl.at[e, side], ysend.at[e, side], yrecv.at[e, side],
                device_id={"gy": lax.rem(gy + step, ny)}, device_id_type=MESH,
            ))
            copies[-1].start()
        for copy in copies:
            copy.wait()

    def stencil(src, e, own, dst, finish):
        y_low, y_high = yl[e, 0], yl[e, 1]
        for c in range(count):
            l, x = divmod(c, tile_x)
            f = block(src, c)
            at = slice(l * LANES, (l + 1) * LANES)

            def k(i):
                return coef[i, c : c + 1, :]

            high = block(src, c + 1) if x + 1 < tile_x else xl[e, 1, :, at]
            low = block(src, c - 1) if x else xl[e, 0, :, at]
            total = k(own) * f - k(2) * high - k(3) * low
            after = jnp.where(
                lane == LANES - 1, pltpu.roll(y_high, LANES - 1 - c, 1), pltpu.roll(f, LANES - 1, 1)
            )
            ahead = jnp.where(
                lane == 0, pltpu.roll(y_low, LANES - c, 1) if c else y_low, pltpu.roll(f, 1, 1)
            )
            total = total - k(4) * after - k(5) * ahead
            if l + 1 < layers:
                total = total - k(6) * block(src, c + tile_x)
            if l:
                total = total - k(7) * block(src, c - tile_x)
            dst[:, c * LANES : (c + 1) * LANES] = finish(c, total)

    def start_all(send, land, e, ssem, rsem, axis, me, n):
        copies = []
        for j in range(1, n):
            copies.append(pltpu.make_async_remote_copy(
                send.at[e], land.at[e, j], ssem.at[e, j], rsem.at[e, j],
                device_id={axis: lax.rem(me + j, n)}, device_id_type=MESH,
            ))
            copies[-1].start()
        return copies

    def finish_all(copies, own, land, e, n):
        for copy in copies:
            copy.wait()
        total = own
        for j in range(1, n):
            total = total + land[e, j]
        return total

    def update(dst, base, coefs, field, sign):
        for c in range(layers):
            at = slice(c * tile_x * LANES, (c + 1) * tile_x * LANES)
            term = small(coefs, field[:, at], TN)
            dst[:, at] = base[:, at] + term if sign > 0 else base[:, at] - term

    v[...] = v_in[...]
    eye = (rows_iota(size, size) == lax.broadcasted_iota(jnp.int32, (size, size), 1)).astype(F32)
    pad = jnp.zeros((size, LANES - 3 * size), F32)

    def time_step(step, carry):
        e = step * (ITERS + 1)
        exchange(v, e)

        def residual_of(c, total):
            if c < tile_x:
                total = total + inj[pl.ds(pl.multiple_of(step * size, size), size),
                                    c * LANES : (c + 1) * LANES]
            return -total

        stencil(v, e, 1, r, residual_of)
        norm = None
        for sweep in range(ITERS):
            direction = d if sweep else r
            e = step * (ITERS + 1) + sweep + 1
            g = step * ITERS + sweep
            exchange(direction, e)
            stencil(direction, e, 0, image, lambda c, total: total)
            curve = small(direction[...], image[...], NT)
            if sweep + 1 < ITERS:
                square = small(image[...], image[...], NT)
                other = small(r[...], image[...] if sweep else r[...], NT)
                own = jnp.concatenate([curve, other, square, pad], axis=1)
            else:
                own = jnp.concatenate([curve, jnp.zeros((size, LANES - size), F32)], axis=1)
            gs[g] = own
            copies = start_all(gs, gl, g, gsend, grecv, "gx", gx, nx)
            inverse = None
            if sweep and sweep + 1 < ITERS:
                (inverse,) = eliminate([beside(norm, eye)])
            own = finish_all(copies, own, gl, g, nx)
            hs[g] = own
            copies = start_all(hs, hl, g, hsend, hrecv, "gy", gy, ny)
            total = finish_all(copies, own, hl, g, ny)
            curve = total[:, :size]
            cross = total[:, size : 2 * size]
            square = total[:, 2 * size : 3 * size]
            if sweep == 0:
                norm, cross = cross, curve
                solved, inverse = eliminate([beside(curve, norm), beside(norm, eye)])
            else:
                (solved,) = eliminate([beside(curve, norm)])
            step_coef = solved[:, size : 2 * size]
            update(v, v, step_coef, direction, 1)
            update(r, r, step_coef, image, -1) if sweep else None
            if sweep + 1 < ITERS:
                cross_term = small(cross, step_coef)
                cross_flip = small(step_coef, cross, (((0,), (1,)), ((), ())))
                square_term = small(step_coef, small(square, step_coef), TN)
                new = norm - cross_term - cross_flip + square_term
                turn = small(inverse[:, size : 2 * size], new)
                if sweep:
                    update(d, r, turn, d, 1)
                else:
                    update(d, r, turn, r, 1)
                    update(d, d, step_coef, image, -1)
                    update(r, r, step_coef, image, -1)
                norm = new
        return carry

    lax.fori_loop(0, steps, time_step, 0)


def solve_grid(nx, ny, steps, layers, tile_x, volts, injected, coef):
    size, width = volts.shape
    halos, grams = steps * (ITERS + 1), steps * ITERS
    dma = pltpu.SemaphoreType.DMA
    return pl.pallas_call(
        functools.partial(grid_kernel, nx, ny, steps, layers, tile_x),
        out_shape=[jax.ShapeDtypeStruct(volts.shape, F32)] * 2,
        in_specs=[pl.BlockSpec(memory_space=pltpu.VMEM)] * 3,
        out_specs=[pl.BlockSpec(memory_space=pltpu.VMEM)] * 2,
        scratch_shapes=[
            pltpu.VMEM(volts.shape, F32),
            pltpu.VMEM(volts.shape, F32),
            pltpu.VMEM((halos, 2, size, layers * LANES), F32),
            pltpu.VMEM((halos, 2, size, layers * LANES), F32),
            pltpu.VMEM((halos, 2, size, LANES), F32),
            pltpu.VMEM((halos, 2, size, LANES), F32),
            pltpu.VMEM((grams, size, LANES), F32),
            pltpu.VMEM((grams, nx, size, LANES), F32),
            pltpu.VMEM((grams, size, LANES), F32),
            pltpu.VMEM((grams, ny, size, LANES), F32),
            dma((halos, 2)), dma((halos, 2)), dma((halos, 2)), dma((halos, 2)),
            dma((grams, nx)), dma((grams, nx)), dma((grams, ny)), dma((grams, ny)),
        ],
        compiler_params=pltpu.CompilerParams(
            collective_id=0, has_side_effects=True, vmem_limit_bytes=48 * 1024 * 1024
        ),
        name="grid",
    )(volts, injected, coef)


def shifted(x, axis):
    length = lax.axis_size(axis)
    return lax.ppermute(x, axis, [(i, i + 1) for i in range(length - 1)])


def body(volts, cap, cond_x, cond_y, via, waveforms, placement, cells, wave_ids, amps):
    nx, ny = lax.axis_size("gx"), lax.axis_size("gy")
    devices = nx * ny
    scenarios, layers, tile_x, tile_y = volts.shape
    steps = waveforms.shape[0] // scenarios
    capacity = 2 * cells.shape[0] // devices
    slots = bin_instances(devices, capacity, placement[:, 0], cells, wave_ids, amps)
    arrived = lax.all_to_all(
        slots.reshape(2, devices, capacity), ("gx", "gy"), split_axis=1, concat_axis=1, tiled=True
    )
    injected = inject(arrived, waveforms, tile_x * tile_y)
    rim_x = shifted(cond_x[:, -1:, :], "gx")
    rim_y = shifted(cond_y[:, :, -1:], "gy")
    x_low = jnp.concatenate([rim_x, cond_x[:, :-1, :]], axis=1)
    y_low = jnp.concatenate([rim_y, cond_y[:, :, :-1]], axis=2)
    via_low = jnp.concatenate([jnp.zeros_like(via[:1]), via[:-1]], axis=0)
    at_x = lax.broadcasted_iota(jnp.int32, cond_x.shape, 1) + lax.axis_index("gx") * tile_x
    at_y = lax.broadcasted_iota(jnp.int32, cond_y.shape, 2) + lax.axis_index("gy") * tile_y
    x_next = jnp.where(at_x == nx * tile_x - 1, 0.0, cond_x)
    y_next = jnp.where(at_y == ny * tile_y - 1, 0.0, cond_y)
    around = cond_x + x_low + cond_y + y_low + via + via_low
    coef = jnp.stack([cap + around, around, x_next, x_low, y_next, y_low, via, via_low])
    coef = coef.reshape(8, layers * tile_x, tile_y)
    out, residual = solve_grid(
        nx, ny, steps, layers, tile_x, volts.reshape(scenarios, -1), injected, coef
    )
    return out.reshape(volts.shape), residual.reshape(volts.shape)


def solution(mesh):
    grid = P(None, "gx", "gy")
    field = P(None, None, "gx", "gy")
    flat = P(("gx", "gy"))
    return jax.shard_map(
        body,
        mesh=mesh,
        in_specs=(field, grid, grid, grid, grid, P(), P(("gx", "gy"), None), flat, flat, flat),
        out_specs=(field, field),
        check_vma=False,
    )
```
